256 devices in a mesh: row: 64 (over z, y, x_hi), col: 2 (over core), depth: 2 (over x_lo).
Axes of the slice: x: 4 (x_hi: 2, x_lo: 2; x = x_hi * 2 + x_lo), y: 4, z: 8, core: 2. Of those that a mesh axis runs over, the one named last changes fastest.
Arguments:
- student_hidden: bfloat16 [16384, 768], P('row', ('depth', 'col')), may hold values from -16 to 16
- embedding: bfloat16 [50304, 768], P('col', ('depth', 'row')), as said below
- teacher_logits: bfloat16 [16384, 50304], P('row', ('col', 'depth')), may hold values from -24 to 124, as said below
Outputs:
- loss: float32 [16384], P('row')
- peak_logprob: float32 [16384], P('row')
The draws below stay inside these ranges and needn't reach their ends.
Inputs may be any that keep to these rules, and one draw needn't show every extreme that they name: embedding entries lie within plus or minus 4 / sqrt(768). teacher_logits lie within -24 and 124; each token's logits carry an offset of 0 to 100.
All inputs are finite; a program needn't handle non-finite values.
Results may differ from the reference program's by a relative error of at most 0.0003.
Values may be sent and summed in bfloat16 or wider, within the bound.
No kernel may reach another device: no remote copies, remote signals or barrier semaphores. Data moves between devices by JAX's collectives and lax.ppermute only.
A program may use at most 128 MiB of HBM per device.

```python
import jax
import jax.numpy as jnp
from jax import lax

D = 768
VOCAB = 50304
TOK_DEV = 256
TOKENS = 16384
N_ROW = 64


def embedding_table(key):
    base = jax.random.normal(jax.random.fold_in(key, 101), (VOCAB, D), jnp.float32)
    return jnp.clip(base, -4.0, 4.0) * D ** (-0.5)


def draw_embedding(key, part):
    return embedding_table(key).astype(jnp.bfloat16)


def draw_student_hidden(key, part):
    hidden = jnp.clip(jax.random.normal(jax.random.fold_in(key, 205), (TOKENS, D), jnp.float32), -6.0, 6.0)
    return jnp.clip(hidden, -16.0, 16.0).astype(jnp.bfloat16)


def draw_teacher_logits(key, part):
    offsets = jax.random.uniform(jax.random.fold_in(key, 301), (TOKENS, 1), jnp.float32, 0.0, 100.0)
    noise = 4.0 * jnp.clip(jax.random.normal(jax.random.fold_in(key, 304), (TOKENS, VOCAB), jnp.float32), -6.0, 6.0)
    return (offsets + noise).astype(jnp.bfloat16)


def setup_inputs(seed: int = 0) -> dict:
    streams_of = jax.random.split(jax.random.key(seed), 4)
    student_hidden = draw_student_hidden(jax.random.fold_in(streams_of[3], 71), 0)
    embedding = draw_embedding(jax.random.fold_in(streams_of[3], 71), 0)
    teacher_logits = draw_teacher_logits(jax.random.fold_in(streams_of[3], 71), 0)
    return {"student_hidden": student_hidden, "embedding": embedding, "teacher_logits": teacher_logits}


def reference(student_hidden, embedding, teacher_logits):
    def token_block(pair):
        hidden_rows, teacher_rows = pair
        student = jnp.dot(hidden_rows, embedding.T, preferred_element_type=jnp.float32)
        teacher_values = teacher_rows.astype(jnp.float32)
        student_peak = jnp.max(student, axis=1)
        teacher_peak = jnp.max(teacher_values, axis=1)
        student_sum = jnp.sum(jnp.exp(student - student_peak[:, None]), axis=1)
        weights = jnp.exp(teacher_values - teacher_peak[:, None])
        teacher_sum = jnp.sum(weights, axis=1)
        cross_sum = jnp.sum(weights * student, axis=1)
        norm_log = jnp.log(student_sum)
        return student_peak + norm_log - cross_sum / teacher_sum, -norm_log

    losses, peaks = lax.map(token_block, (student_hidden.reshape(N_ROW, TOK_DEV, D), teacher_logits.reshape(N_ROW, TOK_DEV, VOCAB)))
    return losses.reshape(TOKENS), peaks.reshape(TOKENS)
```

```python
import jax
import jax.numpy as jnp
from jax import lax
from jax.experimental import pallas as pl
from jax.experimental.pallas import tpu as pltpu
from jax.sharding import Mesh, PartitionSpec as P

HALF = 6288
WIDTHS = ((512,) * 6, (512,) * 6 + (256,))
PARTS = tuple(sum(widths) for widths in WIDTHS)
ROWS = 64
LOW = -3.0e38
FLOW = (1, 0)


def shifted(axis, by):
    count = lax.axis_size(axis)
    return [(i, (i + by) % count) for i in range(count)]


def paired(count, mask):
    return [(i, i ^ mask) for i in range(count)]


def along(value, axis, by):
    return lax.ppermute(value, axis, shifted(axis, by))


def across(value, mask):
    return lax.ppermute(value, ("xh", "depth"), paired(4, mask))


def join_kernel(*refs):
    target, at = refs[-1], 0
    for piece in refs[:-1]:
        rows = piece.shape[0]
        target[at : at + rows, :] = piece[...]
        at += rows


NEAR = pl.BlockSpec(memory_space=pltpu.VMEM)


def joined(pieces):
    rows = sum(piece.shape[0] for piece in pieces)
    return pl.pallas_call(
        join_kernel,
        out_shape=jax.ShapeDtypeStruct((rows, pieces[0].shape[1]), pieces[0].dtype),
        in_specs=[NEAR] * len(pieces),
        out_specs=NEAR,
        compiler_params=pltpu.CompilerParams(vmem_limit_bytes=2 * 2**20),
        name="join",
    )(*pieces)


def cut_kernel(first_ref, second_ref, low_ref, high_ref):
    half = low_ref.shape[0]
    low_ref[...] = first_ref[:half, :]
    high_ref[...] = second_ref[half:, :]


def cut(first, second):
    half = jax.ShapeDtypeStruct((first.shape[0] // 2, first.shape[1]), first.dtype)
    return pl.pallas_call(
        cut_kernel,
        out_shape=[half, half],
        in_specs=[NEAR, NEAR],
        out_specs=[NEAR, NEAR],
        compiler_params=pltpu.CompilerParams(vmem_limit_bytes=2 * 2**20),
        name="cut",
    )(first, second)


def gather_y_then_z(block):
    pieces = [block] + [along(block, "y", k) for k in (1, 2, 3)]
    wide = joined(pieces)
    up, down = [wide], [wide]
    for _ in range(3):
        up.append(along(up[-1], "z", 1))
        down.append(along(down[-1], "z", -1))
    low, high = cut(up[3], down[3])
    return up + [along(low, "z", 1), along(high, "z", -1)] + down[:0:-1]


def gather_z_then_y(block):
    up, down = ([along(block, "z", s * k) for k in (1, 2)] for s in (1, -1))
    up.append(along(up[1], "z", 1))
    down.append(along(down[1], "z", -1))
    far = [along(up[1][:16], "z", 2), along(down[1][16:], "z", -2)]
    wide = joined([block] + up + far + down[::-1])
    one = along(wide, "y", 1)
    three = along(wide, "y", -1)
    low, high = cut(one, three)
    return [wide, one, along(low, "y", 1), along(high, "y", -1), three]


def feature_kernel(near_ref, far_ref, z_first_ref, y_first_ref, held):
    z, y = lax.axis_index("z"), lax.axis_index("y")
    xh, depth, col = lax.axis_index("xh"), lax.axis_index("depth"), lax.axis_index("col")
    for kx in range(4):
        for j, ref in enumerate((near_ref, far_ref)):
            at, tokens = (kx & 1) * 384 + j * 192, (kx >> 1) * 256
            held[at : at + 192, tokens : tokens + 256] = ref[kx * 192 : kx * 192 + 192, :]

    def in_sixes(k):
        return (k * 10923) >> 16

    k = lax.broadcasted_iota(jnp.int32, (768, 1), 0)
    sixth = in_sixes(k)
    j, kx, rest = k - sixth * 6, sixth & 3, sixth >> 2
    line = lax.broadcasted_iota(jnp.int32, (1, 768), 1)
    stretch = in_sixes(line) >> 5
    stored = line - stretch * 192 + (depth ^ (stretch >> 1)) * 384 + (col ^ (stretch & 1)) * 192
    for out_ref, kz, ky in (
        (z_first_ref, rest >> 2, rest & 3),
        (y_first_ref, rest & 7, rest >> 3),
    ):
        owner = ((z - kz) & 7) * 8 + ((y - ky) & 3) * 2 + (xh ^ (kx >> 1))
        wanted = ((depth ^ (kx & 1)) * 64 + owner) * 6 + j
        chosen = jnp.where(wanted == stored, 1.0, 0.0).astype(jnp.bfloat16)
        picked = jnp.dot(chosen, held[...], preferred_element_type=jnp.float32)
        out_ref[...] = picked.T.astype(jnp.bfloat16)


def ordered_features(near, far):
    features = jax.ShapeDtypeStruct((512, 768), jnp.bfloat16)
    return pl.pallas_call(
        feature_kernel,
        out_shape=[features, features],
        in_specs=[NEAR, NEAR],
        out_specs=[NEAR, NEAR],
        scratch_shapes=[pltpu.VMEM((768, 512), jnp.bfloat16)],
        compiler_params=pltpu.CompilerParams(vmem_limit_bytes=8 * 2**20),
        name="features",
    )(near, far)


STRIP = 256


def half_rows(source_ref, low, valid, other):
    if low is None:
        return source_ref
    side = lax.axis_index("xh")
    side = 1 - side if other else side
    return source_ref.at[pl.ds(pl.multiple_of(side * HALF + low, 16), valid)]


def give_kernel(low, source_ref, out_ref, sem):
    copy = pltpu.make_async_copy(half_rows(source_ref, low, out_ref.shape[0], True), out_ref, sem)
    copy.start()
    copy.wait()


def given(low, rows, source):
    return pl.pallas_call(
        lambda *refs: give_kernel(low, *refs),
        out_shape=jax.ShapeDtypeStruct((rows, 256), source.dtype),
        in_specs=[pl.BlockSpec(memory_space=pltpu.HBM)],
        out_specs=NEAR,
        scratch_shapes=[pltpu.SemaphoreType.DMA],
        compiler_params=pltpu.CompilerParams(vmem_limit_bytes=3 * 2**20),
        name="give",
    )(source)


def weight_kernel(valid, low, source_ref, weights_ref, lines_ref, held, sem):
    count = held.shape[0]
    source = half_rows(source_ref, low, valid, False)
    copy = pltpu.make_async_copy(source, held.at[pl.ds(0, valid)], sem)
    copy.start()
    if count > valid:
        held[valid:, :] = jnp.full((count - valid, 256), LOW, jnp.bfloat16)
    copy.wait()

    def higher(r, top):
        strip = held[pl.ds(pl.multiple_of(r * STRIP, STRIP), STRIP), :]
        return jnp.maximum(top, jnp.max(strip.astype(jnp.float32), axis=0, keepdims=True))

    top = lax.fori_loop(0, count // STRIP, higher, jnp.full((1, 256), LOW, jnp.float32))

    def weigh(r, total):
        at = pl.ds(pl.multiple_of(r * STRIP, STRIP), STRIP)
        weights = jnp.exp(held[at, :].astype(jnp.float32) - top)
        weights_ref[:, at] = weights.T
        return total + jnp.sum(weights, axis=0, keepdims=True)

    total = lax.fori_loop(0, count // STRIP, weigh, jnp.zeros((1, 256), jnp.float32))
    lines_ref[0:1, :] = top
    lines_ref[1:2, :] = total


def teacher_weights(count, valid, low, source):
    return pl.pallas_call(
        lambda *refs: weight_kernel(valid, low, *refs),
        out_shape=[
            jax.ShapeDtypeStruct((256, count), jnp.float32),
            jax.ShapeDtypeStruct((2, 256), jnp.float32),
        ],
        in_specs=[pl.BlockSpec(memory_space=pltpu.HBM)],
        out_specs=[NEAR, NEAR],
        scratch_shapes=[pltpu.VMEM((count, 256), jnp.bfloat16), pltpu.SemaphoreType.DMA],
        compiler_params=pltpu.CompilerParams(vmem_limit_bytes=4 * 2**20),
        name="weights",
    )(source)


def tile_terms(low, width, limit, logits_ref, weight_refs, state_ref):
    lane = lax.broadcasted_iota(jnp.int32, (ROWS, 128), 1)
    for first in range(0, 512, ROWS):
        rows, half = pl.ds(first, ROWS), pl.ds(first % 256, ROWS)
        weights_ref = weight_refs[first // 256]

        def shown(at):
            logits = logits_ref[rows, at : at + 128]
            if limit is not None and at + 128 > limit:
                logits = jnp.where(lane < limit - at, logits, LOW)
            return logits

        old = state_ref[0, rows, :]
        top = old
        for at in range(0, width, 128):
            top = jnp.maximum(top, shown(at))
        total, cross = state_ref[1, rows, :] * jnp.exp(old - top), state_ref[2, rows, :]
        for at in range(0, width, 128):
            total += jnp.exp(shown(at) - top)
            cross += weights_ref[half, low + at : low + at + 128] * logits_ref[rows, at : at + 128]
        state_ref[0, rows, :], state_ref[1, rows, :], state_ref[2, rows, :] = top, total, cross


def summary(r, state_ref, other_ref, packed_ref):
    rows = pl.ds(r * ROWS, ROWS)
    student_top = state_ref[0, rows, :]
    student_peak = jnp.max(student_top, axis=1, keepdims=True)
    columns = (
        student_peak,
        jnp.sum(state_ref[1, rows, :] * jnp.exp(student_top - student_peak), axis=1, keepdims=True),
        jnp.sum(other_ref[2, rows, :], axis=1, keepdims=True),
        jnp.sum(state_ref[2, rows, :], axis=1, keepdims=True),
    )
    lane = lax.broadcasted_iota(jnp.int32, (ROWS, 128), 1)
    packed = jnp.zeros((ROWS, 128), jnp.float32)
    for k, column in enumerate(columns):
        packed = jnp.where(lane == k, column, packed)
    packed_ref[rows, :] = packed


def each_block(body):
    def step(r, _):
        body(r)
        return 0

    lax.fori_loop(0, 512 // ROWS, step, 0)


def vocabulary_kernel(pieces, widths, limit, last, *refs):
    piece_refs, refs = refs[:pieces], refs[pieces:]
    weight_refs, features_ref, refs = refs[:2], refs[2], refs[3:]
    if last:
        before_ref, out_ref, line_refs = refs[0], refs[5], refs[1:5]
    else:
        out_ref = refs[0]
    tables, products, state_ref, packed_ref = refs[-6:-4], refs[-4:-2], refs[-2], refs[-1]

    if last:
        state_ref[:2] = before_ref[:2]
    else:
        state_ref[0] = jnp.full((512, 128), LOW, jnp.float32)
        state_ref[1] = jnp.zeros((512, 128), jnp.float32)
    state_ref[2] = jnp.zeros((512, 128), jnp.float32)

    def multiply(step):
        low, width, table, at = sum(widths[:step]), widths[step], tables[step % 2], 0
        for piece in piece_refs:
            rows = piece.shape[0]
            table[at : at + rows, :width] = piece[:, low : low + width]
            at += rows
        products[step % 2][:, :width] = jnp.dot(
            features_ref[...], table[:, :width], preferred_element_type=jnp.float32
        )

    multiply(0)
    for step, width in enumerate(widths):
        final = step + 1 == len(widths)
        if not final:
            multiply(step + 1)
        bound = limit if final else None
        tile_terms(sum(widths[:step]), width, bound, products[step % 2], weight_refs, state_ref)

    if not last:
        out_ref[...] = state_ref[...]
        return
    each_block(lambda r: summary(r, state_ref, before_ref, packed_ref))
    lines = packed_ref[...].T
    xh = lax.axis_index("xh")
    for side in range(2):
        at = slice(side * 256, side * 256 + 256)
        first_ref, second_ref = line_refs[side], line_refs[2 + side]
        top = jnp.maximum(first_ref[:1], second_ref[:1])
        first_scale, second_scale = jnp.exp(first_ref[:1] - top), jnp.exp(second_ref[:1] - top)
        teacher_sum = first_ref[1:2] * first_scale + second_ref[1:2] * second_scale
        cross = lines[2:3, at] * first_scale + lines[3:4, at] * second_scale
        for k in range(4):
            out = out_ref.at[(xh ^ side) * 4 + k]
            out[0:2, :] = lines[0:2, at]
            out[2:3, :], out[3:4, :], out[4:5, :] = top, teacher_sum, cross


def over_vocabulary(part, pieces, features, weights, valid, *before):
    last, widths = bool(before), WIDTHS[part]
    limit = None if valid == PARTS[part] else valid - sum(widths[:-1])
    widest = max(widths)
    return pl.pallas_call(
        lambda *refs: vocabulary_kernel(len(pieces), widths, limit, last, *refs),
        out_shape=jax.ShapeDtypeStruct((8, 5, 256) if last else (3, 512, 128), jnp.float32),
        in_specs=[NEAR] * (len(pieces) + 3 + len(before)),
        out_specs=NEAR,
        scratch_shapes=[
            pltpu.VMEM((768, widest), jnp.bfloat16),
            pltpu.VMEM((768, widest), jnp.bfloat16),
            pltpu.VMEM((512, widest), jnp.float32),
            pltpu.VMEM((512, widest), jnp.float32),
            pltpu.VMEM((3, 512, 128), jnp.float32),
            pltpu.VMEM((512, 128), jnp.float32),
        ],
        compiler_params=pltpu.CompilerParams(vmem_limit_bytes=10 * 2**20),
        name="vocabulary",
    )(*pieces, *weights, features, *before)


def merged(tops, sums):
    top = jnp.max(tops, axis=0)
    scale = jnp.exp(tops - top)
    return top, [jnp.sum(s * scale, axis=0) for s in sums]


def on_device(student_hidden, embedding, teacher_logits):
    xh, depth = lax.axis_index("xh"), lax.axis_index("depth")
    x = xh * 2 + depth
    cuts = ((0, PARTS[0]), (PARTS[0], HALF))

    by_feature = embedding.T.reshape(6, 2, 2, HALF).transpose(2, 1, 0, 3).reshape(4, 6, HALF)
    by_feature = jnp.pad(by_feature, ((0, 0), (0, 0), (0, sum(PARTS) - HALF)))
    mine = [lax.dynamic_index_in_dim(by_feature, x ^ k, 0, False) for k in range(4)]
    block = jnp.concatenate([mine[0]] + [across(mine[k], k) for k in (1, 2, 3)], axis=0)
    blocks = [block[:, : PARTS[0]], block[:, PARTS[0] :]]

    hidden = student_hidden.T
    from_x = [hidden] + [across(hidden, k) for k in (1, 2, 3)]
    near = joined(from_x)
    other = lax.ppermute(near, "col", paired(2, 1))
    features = ordered_features(near, other)

    by_vocab = teacher_logits.T
    weights, tops, valid = [], [], []
    for part, (low, high) in enumerate(cuts):
        count, rows = PARTS[part], high - low
        give = given(low, rows, by_vocab)
        got = lax.ppermute(give, "xh", paired(2, 1))
        own_side = teacher_weights(count, rows, low, by_vocab)
        far_side = teacher_weights(count, rows, None, got)
        weights.append((own_side[0], far_side[0]))
        tops.append((own_side[1], far_side[1]))
        valid.append(rows)

    pieces = (gather_y_then_z(blocks[0]), gather_z_then_y(blocks[1]))
    before = ()
    for part in FLOW:
        args = (part, pieces[part], features[part], weights[part], valid[part])
        state = over_vocabulary(*args, *before)
        before = (state, *tops[part], *tops[1 - part])

    every = lax.all_to_all(state, ("xh", "col", "depth"), 0, 0, tiled=True)
    student_peak, (student_sum,) = merged(every[:, 0], [every[:, 1]])
    _, (teacher_sum, cross_sum) = merged(every[:, 2], [every[:, 3], every[:, 4]])
    norm_log = jnp.log(student_sum)
    return (student_peak + norm_log - cross_sum / teacher_sum, -norm_log)


def solution(mesh):
    fine = Mesh(mesh.devices.reshape(8, 4, 2, 2, 2), ("z", "y", "xh", "col", "depth"))
    row = ("z", "y", "xh")
    in_specs = (P(row, ("depth", "col")), P("col", ("depth", *row)), P(row, ("col", "depth")))

    return jax.shard_map(
        on_device, mesh=fine, in_specs=in_specs, out_specs=(P(row), P(row)), check_vma=False
    )
```

```python
import jax
import jax.numpy as jnp
from jax import lax
from jax.experimental import pallas as pl
from jax.experimental.pallas import tpu as pltpu
from jax.sharding import Mesh, PartitionSpec as P

HALF = 6288
PARTS = (3072, 3328)
BLOCK = 512
ROWS = 64
LOW = -3.0e38
CENTRE = 54.0


def shifted(axis, by):
    count = lax.axis_size(axis)
    return [(i, (i + by) % count) for i in range(count)]


def paired(count, mask):
    return [(i, i ^ mask) for i in range(count)]


def along(value, axis, by):
    return lax.ppermute(value, axis, shifted(axis, by))


def across(value, mask):
    return lax.ppermute(value, ("xh", "depth"), paired(4, mask))


def join_kernel(*refs):
    target, at = refs[-1], 0
    for piece in refs[:-1]:
        rows = piece.shape[0]
        target[at : at + rows, :] = piece[...]
        at += rows


NEAR = pl.BlockSpec(memory_space=pltpu.VMEM)


def joined(pieces):
    rows = sum(piece.shape[0] for piece in pieces)
    return pl.pallas_call(
        join_kernel,
        out_shape=jax.ShapeDtypeStruct((rows, pieces[0].shape[1]), pieces[0].dtype),
        in_specs=[NEAR] * len(pieces),
        out_specs=NEAR,
        compiler_params=pltpu.CompilerParams(vmem_limit_bytes=2 * 2**20),
        name="join",
    )(*pieces)


def join_halves_kernel(*refs):
    first_ref, second_ref, at = refs[-2], refs[-1], 0
    middle = first_ref.shape[1]
    for piece in refs[:-2]:
        rows = piece.shape[0]
        first_ref[at : at + rows, :] = piece[:, :middle]
        second_ref[at : at + rows, :] = piece[:, middle:]
        at += rows


def joined_halves(pieces):
    rows, columns = sum(piece.shape[0] for piece in pieces), pieces[0].shape[1]
    half = jax.ShapeDtypeStruct((rows, columns // 2), pieces[0].dtype)
    return pl.pallas_call(
        join_halves_kernel,
        out_shape=[half, half],
        in_specs=[NEAR] * len(pieces),
        out_specs=[NEAR, NEAR],
        compiler_params=pltpu.CompilerParams(vmem_limit_bytes=2 * 2**20),
        name="join",
    )(*pieces)


def cut_kernel(first_ref, second_ref, low_ref, high_ref):
    half = low_ref.shape[0]
    low_ref[...] = first_ref[:half, :]
    high_ref[...] = second_ref[half:, :]


def cut(first, second):
    half = jax.ShapeDtypeStruct((first.shape[0] // 2, first.shape[1]), first.dtype)
    return pl.pallas_call(
        cut_kernel,
        out_shape=[half, half],
        in_specs=[NEAR, NEAR],
        out_specs=[NEAR, NEAR],
        compiler_params=pltpu.CompilerParams(vmem_limit_bytes=2 * 2**20),
        name="cut",
    )(first, second)


def gather_y_then_z(block):
    pieces = [block] + [along(block, "y", k) for k in (1, 2, 3)]
    halves = joined_halves(pieces)
    gathered = []
    for name, wide in zip("PQ", halves):
        up, down = [wide], [wide]
        for _ in range(3):
            up.append(along(up[-1], "z", 1))
            down.append(along(down[-1], "z", -1))
        last, by = (up[3], 1) if name == "P" else (down[3], -1)
        gathered.append(up + [along(last, "z", by)] + down[:0:-1])
    return gathered


def gather_z_then_y(block):
    up, down = ([along(block, "z", s * k) for k in (1, 2)] for s in (1, -1))
    up.append(along(up[1], "z", 1))
    down.append(along(down[1], "z", -1))
    far = [along(up[1][:16], "z", 2), along(down[1][16:], "z", -2)]
    wide = joined([block] + up + far + down[::-1])
    one = along(wide, "y", 1)
    three = along(wide, "y", -1)
    low, high = cut(one, three)
    return [wide, one, along(low, "y", 1), along(high, "y", -1), three]


def feature_kernel(near_ref, far_ref, z_first_ref, y_first_ref, held):
    z, y = lax.axis_index("z"), lax.axis_index("y")
    xh, depth, col = lax.axis_index("xh"), lax.axis_index("depth"), lax.axis_index("col")
    for kx in range(4):
        for j, ref in enumerate((near_ref, far_ref)):
            at, tokens = (kx & 1) * 384 + j * 192, (kx >> 1) * 256
            held[at : at + 192, tokens : tokens + 256] = ref[kx * 192 : kx * 192 + 192, :]

    def in_sixes(k):
        return (k * 10923) >> 16

    k = lax.broadcasted_iota(jnp.int32, (768, 1), 0)
    sixth = in_sixes(k)
    j, kx, rest = k - sixth * 6, sixth & 3, sixth >> 2
    line = lax.broadcasted_iota(jnp.int32, (1, 768), 1)
    stretch = in_sixes(line) >> 5
    stored = line - stretch * 192 + (depth ^ (stretch >> 1)) * 384 + (col ^ (stretch & 1)) * 192
    for out_ref, kz, ky in (
        (z_first_ref, rest >> 2, rest & 3),
        (y_first_ref, rest & 7, rest >> 3),
    ):
        owner = ((z - kz) & 7) * 8 + ((y - ky) & 3) * 2 + (xh ^ (kx >> 1))
        wanted = ((depth ^ (kx & 1)) * 64 + owner) * 6 + j
        chosen = jnp.where(wanted == stored, 1.0, 0.0).astype(jnp.bfloat16)
        picked = jnp.dot(chosen, held[...], preferred_element_type=jnp.float32)
        out_ref[...] = picked.T.astype(jnp.bfloat16)


def ordered_features(near, far):
    features = jax.ShapeDtypeStruct((512, 768), jnp.bfloat16)
    return pl.pallas_call(
        feature_kernel,
        out_shape=[features, features],
        in_specs=[NEAR, NEAR],
        out_specs=[NEAR, NEAR],
        scratch_shapes=[pltpu.VMEM((768, 512), jnp.bfloat16)],
        compiler_params=pltpu.CompilerParams(vmem_limit_bytes=8 * 2**20),
        name="features",
    )(near, far)


STRIP = 256


def half_rows(source_ref, low, valid, other):
    if low is None:
        return source_ref
    side = lax.axis_index("xh")
    side = 1 - side if other else side
    return source_ref.at[pl.ds(pl.multiple_of(side * HALF + low, 16), valid)]


def split_kernel(table_ref, *refs):
    held = refs[-1]
    x = lax.axis_index("xh") * 2 + lax.axis_index("depth")
    table = table_ref[...]
    for part in range(4):
        to = (part & 1) * 2 + (part >> 1)
        held[to, :, HALF:] = jnp.zeros((6, sum(PARTS) - HALF), table.dtype)
        held[to, :, :HALF] = table[:, part * HALF : (part + 1) * HALF]
    for k, out_ref in enumerate(refs[:-1]):
        out_ref[...] = held[x ^ k]


def split_table(table):
    part = jax.ShapeDtypeStruct((6, sum(PARTS)), table.dtype)
    return pl.pallas_call(
        split_kernel,
        out_shape=[part] * 4,
        in_specs=[NEAR],
        out_specs=[NEAR] * 4,
        scratch_shapes=[pltpu.VMEM((4, 6, sum(PARTS)), table.dtype)],
        compiler_params=pltpu.CompilerParams(vmem_limit_bytes=6 * 2**20),
        name="split",
    )(table)


def give_kernel(low, source_ref, out_ref, sem):
    copy = pltpu.make_async_copy(half_rows(source_ref, low, out_ref.shape[0], True), out_ref, sem)
    copy.start()
    copy.wait()


def given(low, rows, source):
    return pl.pallas_call(
        lambda *refs: give_kernel(low, *refs),
        out_shape=jax.ShapeDtypeStruct((rows, 256), source.dtype),
        in_specs=[pl.BlockSpec(memory_space=pltpu.HBM)],
        out_specs=NEAR,
        scratch_shapes=[pltpu.SemaphoreType.DMA],
        compiler_params=pltpu.CompilerParams(vmem_limit_bytes=3 * 2**20),
        cost_estimate=pl.CostEstimate(flops=0, bytes_accessed=1024, transcendentals=0),
        name="give",
    )(source)


def weight_kernel(valid, low, source_ref, weights_ref, held, sem):
    count = held.shape[0]
    source = half_rows(source_ref, low, valid, False)
    copy = pltpu.make_async_copy(source, held.at[pl.ds(0, valid)], sem)
    copy.start()
    if count > valid:
        held[valid:, :] = jnp.full((count - valid, 256), LOW, jnp.bfloat16)
    copy.wait()

    def weigh(r, _):
        at = pl.ds(pl.multiple_of(r * STRIP, STRIP), STRIP)
        weights_ref[:, at] = jnp.exp(held[at, :].T.astype(jnp.float32) - CENTRE)
        return 0

    lax.fori_loop(0, count // STRIP, weigh, 0)


def teacher_weights(count, valid, low, source):
    return pl.pallas_call(
        lambda *refs: weight_kernel(valid, low, *refs),
        out_shape=jax.ShapeDtypeStruct((256, count), jnp.float32),
        in_specs=[pl.BlockSpec(memory_space=pltpu.HBM)],
        out_specs=NEAR,
        scratch_shapes=[pltpu.VMEM((count, 256), jnp.bfloat16), pltpu.SemaphoreType.DMA],
        compiler_params=pltpu.CompilerParams(vmem_limit_bytes=4 * 2**20),
        name="weights",
    )(source)


def tile_terms(low, width, limit, logits_ref, weight_refs, state_ref):
    lane = lax.broadcasted_iota(jnp.int32, (ROWS, 128), 1)
    for first in range(0, 512, ROWS):
        rows, half = pl.ds(first, ROWS), pl.ds(first % 256, ROWS)
        weights_ref = weight_refs[first // 256]

        def shown(at):
            logits = logits_ref[rows, at : at + 128]
            if limit is not None and at + 128 > limit:
                logits = jnp.where(lane < limit - at, logits, LOW)
            return logits

        old = state_ref[0, rows, :]
        top = old
        for at in range(0, width, 128):
            top = jnp.maximum(top, shown(at))
        total = state_ref[1, rows, :] * jnp.exp(old - top)
        weight_sum, cross = state_ref[2, rows, :], state_ref[3, rows, :]
        for at in range(0, width, 128):
            weights = weights_ref[half, low + at : low + at + 128]
            total += jnp.exp(shown(at) - top)
            weight_sum += weights
            cross += weights * logits_ref[rows, at : at + 128]
        for k, value in enumerate((top, total, weight_sum, cross)):
            state_ref[k, rows, :] = value


def summary(r, state_ref, packed_ref):
    rows = pl.ds(r * ROWS, ROWS)
    student_top = state_ref[0, rows, :]
    student_peak = jnp.max(student_top, axis=1, keepdims=True)
    columns = (
        student_peak,
        jnp.sum(state_ref[1, rows, :] * jnp.exp(student_top - student_peak), axis=1, keepdims=True),
        jnp.sum(state_ref[2, rows, :], axis=1, keepdims=True),
        jnp.sum(state_ref[3, rows, :], axis=1, keepdims=True),
    )
    lane = lax.broadcasted_iota(jnp.int32, (ROWS, 128), 1)
    packed = jnp.zeros((ROWS, 128), jnp.float32)
    for k, column in enumerate(columns):
        packed = jnp.where(lane == k, column, packed)
    packed_ref[rows, :] = packed


def each_block(body):
    def step(r, _):
        body(r)
        return 0

    lax.fori_loop(0, 512 // ROWS, step, 0)


def vocabulary_kernel(pieces, widths, offset, limit, place, *refs):
    piece_refs, refs = refs[:pieces], refs[pieces:]
    weight_refs, features_ref, refs = refs[:2], refs[2], refs[3:]
    first, last = place == "first", place == "last"
    tables, products, state_ref, packed_ref = refs[-6:-4], refs[-4:-2], refs[-2], refs[-1]
    if first:
        out_ref = refs[0]
        state_ref[...] = jnp.zeros((4, 512, 128), jnp.float32)
        state_ref[0] = jnp.full((512, 128), LOW, jnp.float32)
    else:
        state_ref[...] = refs[0][...]
        out_ref = refs[1]

    def multiply(step):
        low, width, table, at = sum(widths[:step]), widths[step], tables[step % 2], 0
        for piece in piece_refs:
            rows = piece.shape[0]
            table[at : at + rows, :width] = piece[:, low : low + width]
            at += rows
        products[step % 2][:, :width] = jnp.dot(
            features_ref[...], table[:, :width], preferred_element_type=jnp.float32
        )

    multiply(0)
    for step, width in enumerate(widths):
        final = step + 1 == len(widths)
        if not final:
            multiply(step + 1)
        bound = limit if final else None
        low = offset + sum(widths[:step])
        tile_terms(low, width, bound, products[step % 2], weight_refs, state_ref)

    if not last:
        out_ref[...] = state_ref[...]
        return
    each_block(lambda r: summary(r, state_ref, packed_ref))
    lines = packed_ref[...].T
    xh = lax.axis_index("xh")
    for side in range(2):
        for k in range(4):
            out_ref[(xh ^ side) * 4 + k] = lines[0:4, side * 256 : side * 256 + 256]


def over_vocabulary(offset, valid, place, pieces, features, weights, *before):
    count = pieces[0].shape[1]
    widths = (BLOCK,) * (count // BLOCK) + ((count % BLOCK,) if count % BLOCK else ())
    limit = None if valid >= offset + count else valid - offset - sum(widths[:-1])
    widest = max(widths)
    return pl.pallas_call(
        lambda *refs: vocabulary_kernel(len(pieces), widths, offset, limit, place, *refs),
        out_shape=jax.ShapeDtypeStruct((8, 4, 256) if place == "last" else (4, 512, 128), jnp.float32),
        in_specs=[NEAR] * (len(pieces) + 3 + len(before)),
        out_specs=NEAR,
        scratch_shapes=[
            pltpu.VMEM((768, widest), jnp.bfloat16),
            pltpu.VMEM((768, widest), jnp.bfloat16),
            pltpu.VMEM((512, widest), jnp.float32),
            pltpu.VMEM((512, widest), jnp.float32),
            pltpu.VMEM((4, 512, 128), jnp.float32),
            pltpu.VMEM((512, 128), jnp.float32),
        ],
        compiler_params=pltpu.CompilerParams(vmem_limit_bytes=10 * 2**20),
        name="vocabulary",
    )(*pieces, *weights, features, *before)


def on_device(student_hidden, embedding, teacher_logits):
    cuts = ((0, PARTS[0]), (PARTS[0], HALF))

    mine = split_table(embedding.T)
    block = jnp.concatenate([mine[0]] + [across(mine[k], k) for k in (1, 2, 3)], axis=0)
    blocks = [block[:, : PARTS[0]], block[:, PARTS[0] :]]

    hidden = student_hidden.T
    from_x = [hidden] + [across(hidden, k) for k in (1, 2, 3)]
    near = joined(from_x)
    other = lax.ppermute(near, "col", paired(2, 1))
    features = ordered_features(near, other)

    by_vocab = teacher_logits.T
    weights, valid = [], []
    for part, (low, high) in enumerate(cuts):
        count, rows = PARTS[part], high - low
        give = given(low, rows, by_vocab)
        got = lax.ppermute(give, "xh", paired(2, 1))
        own_side = teacher_weights(count, rows, low, by_vocab)
        far_side = teacher_weights(count, rows, None, got)
        weights.append((own_side, far_side))
        valid.append(rows)

    first, second = gather_y_then_z(blocks[0])
    third = gather_z_then_y(blocks[1])
    middle = PARTS[0] // 2
    state = over_vocabulary(0, valid[0], "first", first, features[0], weights[0])
    state = over_vocabulary(middle, valid[0], "next", second, features[0], weights[0], state)
    state = over_vocabulary(0, valid[1], "last", third, features[1], weights[1], state)

    every = lax.all_to_all(state, ("xh", "col", "depth"), 0, 0, tiled=True)
    student_peak = jnp.max(every[:, 0], axis=0)
    student_sum = jnp.sum(every[:, 1] * jnp.exp(every[:, 0] - student_peak), axis=0)
    teacher_sum, cross_sum = jnp.sum(every[:, 2], axis=0), jnp.sum(every[:, 3], axis=0)
    norm_log = jnp.log(student_sum)
    return (student_peak + norm_log - cross_sum / teacher_sum, -norm_log)


def solution(mesh):
    fine = Mesh(mesh.devices.reshape(8, 4, 2, 2, 2), ("z", "y", "xh", "col", "depth"))
    row = ("z", "y", "xh")
    in_specs = (P(row, ("depth", "col")), P("col", ("depth", *row)), P(row, ("col", "depth")))

    return jax.shard_map(
        on_device, mesh=fine, in_specs=in_specs, out_specs=(P(row), P(row)), check_vma=False
    )
```
